32 devices in a mesh: dp: 1 (over z), tp: 4 (over y), ep: 8 (over x, core).
Axes of the slice: x: 4, y: 4, z: 1, core: 2. Of those that a mesh axis runs over, the one named last changes fastest.
The devices are a block of a 4x4x8 slice.
Arguments:
- tokens: bfloat16 [16384, 2048], P(('dp', 'ep'))
- expert_ids: int32 [16384, 2], P(('dp', 'ep'))
- norm_gain: bfloat16 [2048], replicated
- router_w: bfloat16 [2048, 8], replicated
- w_gate: bfloat16 [8, 2048, 5632], P('ep', None, 'tp')
- w_up: bfloat16 [8, 2048, 5632], P('ep', None, 'tp')
- w_down: bfloat16 [8, 5632, 2048], P('ep', 'tp')
Outputs:
- output: bfloat16 [16384, 2048], P(('dp', 'ep'))
All inputs are finite; a program needn't handle non-finite values.
Results may differ from the reference program's by a relative error of at most 0.014385.
Values are sent between devices in bfloat16 or wider.
A program may use at most 768 MiB of HBM per device.

```python
import jax
import jax.numpy as jnp
from jax import lax

MODEL_DIM = 2048
FFN_DIM = 5632
NUM_EXPERTS = 8
TOP_K = 2
EP_SIZE = 8
TOK_DEV = 2048
TOKENS = EP_SIZE * TOK_DEV
SLOT_CAP = 2 * TOP_K * TOK_DEV // NUM_EXPERTS
EXPERT_CAP = EP_SIZE * SLOT_CAP
NORM_EPS = 1e-5


def route_block(key):
    mean_load = TOP_K * TOK_DEV // NUM_EXPERTS
    key_lift, key_perm, key_tok = jax.random.split(key, 3)
    lifts = jax.random.randint(key_lift, (NUM_EXPERTS,), 1, mean_load, jnp.int32)
    lifts = lifts.at[0].set(mean_load).at[1].set(0)
    loads = mean_load + lifts - jnp.roll(lifts, -1)
    order = jnp.repeat(jnp.arange(NUM_EXPERTS, dtype=jnp.int32), loads, total_repeat_length=TOP_K * TOK_DEV)
    choice = order.reshape(TOP_K, TOK_DEV).T
    relabel = jax.random.permutation(key_perm, NUM_EXPERTS).astype(jnp.int32)
    shuffle = jax.random.permutation(key_tok, TOK_DEV)
    return relabel[choice][shuffle]


def setup_inputs(seed: int = 0, part: int = 0) -> dict:
    keys = jax.random.split(jax.random.key(seed), 5)
    tok_key = jax.random.fold_in(jax.random.key(seed + 1), part)
    route_key = jax.random.fold_in(jax.random.key(seed + 2), part)
    tokens = jax.random.normal(tok_key, (TOKENS, MODEL_DIM), jnp.float32)
    expert_ids = jax.vmap(route_block)(jax.random.split(route_key, EP_SIZE)).reshape(TOKENS, TOP_K)
    norm_gain = 1.0 + 0.5 * jax.random.normal(keys[0], (MODEL_DIM,), jnp.float32)
    router_w = jax.random.normal(keys[1], (MODEL_DIM, NUM_EXPERTS), jnp.float32) * MODEL_DIM ** -0.5
    w_gate = jax.random.normal(keys[2], (NUM_EXPERTS, MODEL_DIM, FFN_DIM), jnp.float32) * MODEL_DIM ** -0.5
    w_up = jax.random.normal(keys[3], (NUM_EXPERTS, MODEL_DIM, FFN_DIM), jnp.float32) * MODEL_DIM ** -0.5
    w_down = jax.random.normal(keys[4], (NUM_EXPERTS, FFN_DIM, MODEL_DIM), jnp.float32) * (2.0 * FFN_DIM ** -0.5)
    return {'tokens': tokens.astype(jnp.bfloat16), 'expert_ids': expert_ids, 'norm_gain': norm_gain.astype(jnp.bfloat16), 'router_w': router_w.astype(jnp.bfloat16), 'w_gate': w_gate.astype(jnp.bfloat16), 'w_up': w_up.astype(jnp.bfloat16), 'w_down': w_down.astype(jnp.bfloat16)}


def expert_ffn(operands):
    rows, gate_mat, up_mat, down_mat = operands
    gate_act = jnp.dot(rows, gate_mat, preferred_element_type=jnp.float32)
    up_act = jnp.dot(rows, up_mat, preferred_element_type=jnp.float32)
    hidden = (jax.nn.silu(gate_act) * up_act).astype(jnp.bfloat16)
    return jnp.dot(hidden, down_mat, preferred_element_type=jnp.float32).astype(jnp.bfloat16)


def reference(tokens, expert_ids, norm_gain, router_w, w_gate, w_up, w_down):
    tok_f32 = tokens.astype(jnp.float32)
    inv_rms = lax.rsqrt(jnp.mean(tok_f32 * tok_f32, axis=-1, keepdims=True) + NORM_EPS)
    normed = (tok_f32 * inv_rms * norm_gain.astype(jnp.float32)).astype(jnp.bfloat16)
    logits = jnp.dot(normed, router_w, preferred_element_type=jnp.float32)
    gates = jax.nn.softmax(jnp.take_along_axis(logits, expert_ids, axis=1), axis=-1)
    flat_ids = expert_ids.reshape(-1)
    onehot = (flat_ids[:, None] == jnp.arange(NUM_EXPERTS, dtype=jnp.int32)[None, :]).astype(jnp.int32)
    slot_ids = jnp.sum(jnp.cumsum(onehot, axis=0) * onehot, axis=1) - 1
    row_tok = jnp.arange(TOKENS * TOP_K, dtype=jnp.int32) // TOP_K
    src_rows = jnp.zeros((NUM_EXPERTS, EXPERT_CAP), jnp.int32).at[flat_ids, slot_ids].set(row_tok)
    buffers = normed[src_rows]
    expert_out = lax.map(expert_ffn, (buffers, w_gate, w_up, w_down))
    picked = expert_out[flat_ids, slot_ids].reshape(TOKENS, TOP_K, MODEL_DIM).astype(jnp.float32)
    mixed = jnp.sum(gates[:, :, None] * picked, axis=1)
    return (tok_f32 + mixed).astype(jnp.bfloat16)
```

```python
import functools

import jax
import jax.numpy as jnp
from jax import lax
from jax.experimental import pallas as pl
from jax.experimental.pallas import tpu as pltpu
from jax.sharding import PartitionSpec as P


NORM_EPS = 1e-5
GROUPS = (((512, 512), True), ((512,), False), ((512,), False))
PIECES = sum((sizes for sizes, _ in GROUPS), ())
CHUNK = 256
ALIGN = 16
WIN = CHUNK + ALIGN
SHARE = 128
ORDER = ("A1", "A2", "F0", "F1", "F2", "S0", "F3", "S1", "S2", "S3", "M0123")
LEVELS = ((1536, 304, (128, True), (192, 2)), (1792, 320, (128, 1), (128, 1)))
SPARE_TILE = 128
LANES = 128


def rms_norm(x_ref, gain_ref):
    x = x_ref[...].astype(jnp.float32)
    inv = lax.rsqrt(jnp.mean(x * x, axis=-1, keepdims=True) + NORM_EPS)
    return (x * inv * gain_ref[...].astype(jnp.float32)).astype(jnp.bfloat16)


def norm_kernel(at_ref, x_ref, gain_ref, h_ref):
    h_ref[...] = rms_norm(x_ref, gain_ref)


def norm_rows(begin, rows, share, tokens, gain, blk=64):
    dim = tokens.shape[1]
    return pl.pallas_call(
        norm_kernel,
        grid_spec=pltpu.PrefetchScalarGridSpec(
            num_scalar_prefetch=1,
            grid=(rows // blk,),
            in_specs=[
                pl.BlockSpec((blk, dim), lambda i, at: (begin // blk + at[0] * (rows // blk) + i, 0)),
                pl.BlockSpec((1, dim), lambda i, at: (0, 0)),
            ],
            out_specs=pl.BlockSpec((blk, dim), lambda i, at: (i, 0)),
        ),
        out_shape=pltpu.HBM((rows, dim), jnp.bfloat16),
        cost_estimate=pl.CostEstimate(flops=8 * rows * dim, bytes_accessed=4 * rows * dim, transcendentals=0),
        name="norm",
    )(share, tokens, gain)


def gate_kernel(x_ref, ids_ref, gain_ref, rw_ref, gate_ref):
    logits = jnp.dot(rms_norm(x_ref, gain_ref), rw_ref[...], preferred_element_type=jnp.float32)
    lane = lax.broadcasted_iota(jnp.int32, logits.shape, 1)
    ids = ids_ref[...]
    l0 = jnp.sum(jnp.where(lane == ids[:, 0:1], logits, 0.0), axis=-1, keepdims=True)
    l1 = jnp.sum(jnp.where(lane == ids[:, 1:2], logits, 0.0), axis=-1, keepdims=True)
    top = jnp.maximum(l0, l1)
    e0, e1 = jnp.exp(l0 - top), jnp.exp(l1 - top)
    tot = e0 + e1
    gate_ref[...] = jnp.where(lane == 0, e0 / tot, jnp.where(lane == 1, e1 / tot, 0.0))


def gate_rows(tokens, ids, gain, rw):
    rows, dim = tokens.shape
    blk = 64
    return pl.pallas_call(
        gate_kernel,
        grid=(rows // blk,),
        in_specs=[
            pl.BlockSpec((blk, dim), lambda i: (i, 0)),
            pl.BlockSpec((blk, ids.shape[1]), lambda i: (i, 0)),
            pl.BlockSpec((1, dim), lambda i: (0, 0)),
            pl.BlockSpec((dim, LANES), lambda i: (0, 0)),
        ],
        out_specs=pl.BlockSpec((blk, LANES), lambda i: (i, 0)),
        out_shape=jax.ShapeDtypeStruct((rows, LANES), jnp.float32),
        cost_estimate=pl.CostEstimate(flops=2 * rows * dim * LANES, bytes_accessed=2 * rows * dim, transcendentals=0),
        name="gate",
    )(tokens, ids, gain, rw)


def ffn_kernel(unroll, tile_rows, rows_of, per_block, meta_ref, pos_ref, hall_ref, w13_hbm, w2_hbm, y_ref,
               w13_ref, w2_ref, rows_s, u_s, hbuf, obuf, wsem, hsem, osem):
    chunks = pos_ref.shape[0]
    nup, _, pair = w13_ref.shape
    half = pair // 2
    ndown, _, wide = w2_ref.shape
    slots = hbuf.shape[0]

    def fetch(j):
        slot = lax.rem(j, slots)
        row = pl.multiple_of((j // per_block) * rows_of[0] + rows_of[1] + lax.rem(j, per_block) * CHUNK, CHUNK)
        return pltpu.make_async_copy(hall_ref.at[pl.ds(row, CHUNK)], hbuf.at[slot], hsem.at[slot])

    for j in range(slots - 1):
        fetch(j).start()
    weights = [pltpu.make_async_copy(w13_hbm, w13_ref, wsem.at[0]), pltpu.make_async_copy(w2_hbm, w2_ref, wsem.at[1])]
    for w in weights:
        w.start()

    def compact(j, carry):
        @pl.when(j + slots - 1 < chunks)
        def _():
            fetch(j + slots - 1).start()

        fetch(j).wait()
        slot = lax.rem(j, slots)
        start = pl.multiple_of(meta_ref[j], ALIGN)
        rel = pos_ref[j] - start
        pick = (lax.broadcasted_iota(jnp.int32, (WIN, CHUNK), 0) == rel).astype(jnp.bfloat16)
        got = jnp.dot(pick, hbuf[slot], preferred_element_type=jnp.float32).astype(jnp.bfloat16)
        old = rows_s[pl.ds(start, ALIGN), :]
        old = jnp.where(lax.rem(j, per_block) == 0, jnp.zeros_like(old), old)
        rows_s[pl.ds(start, ALIGN), :] = old + got[:ALIGN]
        rows_s[pl.ds(start + ALIGN, CHUNK), :] = got[ALIGN:]
        return carry

    lax.fori_loop(0, chunks, compact, 0)
    for w in weights:
        w.wait()

    def put(i):
        slot = lax.rem(i, 2)
        return pltpu.make_async_copy(obuf.at[slot], y_ref.at[pl.ds(pl.multiple_of(i * tile_rows, ALIGN), tile_rows)], osem.at[slot])

    tiles = meta_ref[chunks]

    def tile(i, carry):
        slot = lax.rem(i, 2)
        a = rows_s[pl.ds(pl.multiple_of(i * tile_rows, ALIGN), tile_rows), :]

        def up_step(j, c):
            both = jnp.dot(a, w13_ref[j], preferred_element_type=jnp.float32)
            act, up = both[:, :half], both[:, half:]
            u_s[:, pl.ds(pl.multiple_of(j * half, half), half)] = (jax.nn.silu(act) * up).astype(jnp.bfloat16)
            return c

        lax.fori_loop(0, nup, up_step, 0, unroll=unroll)

        @pl.when(i >= 2)
        def _():
            put(i - 2).wait()

        u = u_s[...]

        def down_step(j, c):
            obuf[slot, :, pl.ds(pl.multiple_of(j * wide, wide), wide)] = jnp.dot(
                u, w2_ref[j], preferred_element_type=jnp.float32
            ).astype(jnp.bfloat16)
            return c

        lax.fori_loop(0, ndown, down_step, 0, unroll=unroll)
        put(i).start()
        return carry

    lax.fori_loop(0, tiles, tile, 0)

    @pl.when(tiles >= 2)
    def _():
        put(tiles - 2).wait()

    @pl.when(tiles >= 1)
    def _():
        put(tiles - 1).wait()


def ffn_piece(unroll, cap, tile_rows, rows_of, per_block, meta, pos, hall, w13, w2):
    dim, width = w13.shape[1], w2.shape[1]
    slots = 4
    hbm = pl.BlockSpec(memory_space=pltpu.HBM)
    vmem = pl.BlockSpec(memory_space=pltpu.VMEM)
    scratch = 2 * dim * (cap + WIN + slots * CHUNK + 2 * tile_rows) + 2 * tile_rows * width
    return pl.pallas_call(
        functools.partial(ffn_kernel, unroll, tile_rows, rows_of, per_block),
        in_specs=[pl.BlockSpec(memory_space=pltpu.SMEM), vmem, hbm, hbm, hbm],
        out_specs=hbm,
        scratch_shapes=[
            pltpu.VMEM(w13.shape, w13.dtype),
            pltpu.VMEM(w2.shape, w2.dtype),
            pltpu.VMEM((cap + WIN, dim), jnp.bfloat16),
            pltpu.VMEM((tile_rows, width), jnp.bfloat16),
            pltpu.VMEM((slots, CHUNK, dim), jnp.bfloat16),
            pltpu.VMEM((2, tile_rows, dim), jnp.bfloat16),
            pltpu.SemaphoreType.DMA((2,)),
            pltpu.SemaphoreType.DMA((slots,)),
            pltpu.SemaphoreType.DMA((2,)),
        ],
        out_shape=pltpu.HBM((cap, dim), jnp.bfloat16),
        compiler_params=pltpu.CompilerParams(vmem_limit_bytes=scratch + 2 * (w13.size + w2.size) + 6 * 1024 * 1024),
        cost_estimate=pl.CostEstimate(
            flops=6 * (cap * 3 // 4) * dim * width, bytes_accessed=2 * (hall.size + cap * dim), transcendentals=0
        ),
        name="ffn",
    )(meta, pos, *(pltpu.with_memory_space_constraint(a, pltpu.HBM) for a in (hall, w13, w2)))


def pair_kernel(w1_ref, w3_ref, out_ref):
    half = w1_ref.shape[1]
    out_ref[0, :, :half] = w1_ref[...]
    out_ref[0, :, half:] = w3_ref[...]


def pair_columns(w1, w3):
    dim, width = w1.shape
    return pl.pallas_call(
        pair_kernel,
        grid=(width // LANES,),
        in_specs=[pl.BlockSpec((dim, LANES), lambda j: (0, j))] * 2,
        out_specs=pl.BlockSpec((1, dim, 2 * LANES), lambda j: (j, 0, 0)),
        out_shape=pltpu.HBM((width // LANES, dim, 2 * LANES), w1.dtype),
        cost_estimate=pl.CostEstimate(flops=8 * dim * width, bytes_accessed=8 * dim * width, transcendentals=0),
        name="pair",
    )(w1, w3)


def block_kernel(w_ref, out_ref):
    out_ref[0] = w_ref[...]


def block_columns(w):
    width, dim = w.shape
    wide = 2 * LANES
    return pl.pallas_call(
        block_kernel,
        grid=(dim // wide,),
        in_specs=[pl.BlockSpec((width, wide), lambda j: (0, j))],
        out_specs=pl.BlockSpec((1, width, wide), lambda j: (j, 0, 0)),
        out_shape=pltpu.HBM((dim // wide, width, wide), w.dtype),
        cost_estimate=pl.CostEstimate(flops=4 * dim * width, bytes_accessed=4 * dim * width, transcendentals=0),
        name="block",
    )(w)


def spread_kernel(cap_slots, meta_ref, y_ref, out_ref):
    blocks = out_ref.shape[0] // cap_slots
    cols = out_ref.shape[1]

    def clear(g, carry):
        out_ref[pl.ds(pl.multiple_of(g * ALIGN, ALIGN), ALIGN), :] = jnp.zeros((ALIGN, cols), out_ref.dtype)
        return carry

    lax.fori_loop(0, out_ref.shape[0] // ALIGN, clear, 0, unroll=8)
    for s in range(blocks):
        def body(g, carry):
            src = pl.multiple_of(meta_ref[s] + g * ALIGN, ALIGN)
            dst = pl.multiple_of(s * cap_slots + g * ALIGN, ALIGN)
            out_ref[pl.ds(dst, ALIGN), :] = y_ref[pl.ds(src, ALIGN), :]
            return carry

        lax.fori_loop(0, meta_ref[blocks + s], body, 0)


def spread_piece(cap_slots, blocks, meta, y):
    cap, cols = y.shape
    return pl.pallas_call(
        functools.partial(spread_kernel, cap_slots),
        grid_spec=pltpu.PrefetchScalarGridSpec(
            num_scalar_prefetch=1,
            grid=(1,),
            in_specs=[pl.BlockSpec((cap, cols), lambda i, m: (0, 0))],
            out_specs=pl.BlockSpec((blocks * cap_slots, cols), lambda i, m: (0, 0)),
        ),
        out_shape=pltpu.HBM((blocks * cap_slots, cols), y.dtype),
        cost_estimate=pl.CostEstimate(flops=1 << 20, bytes_accessed=4 * (cap + blocks * cap_slots) * cols, transcendentals=0),
        name="spread",
    )(meta, y)


def mix_kernel(col_ref, rows_ref, x_ref, slot_ref, gate_ref, out_ref, both_s):
    toks = x_ref.shape[0]
    experts, slots, _ = rows_ref.shape
    lane = lax.broadcasted_iota(jnp.int32, (toks, slots), 1)
    q = slot_ref[...]
    both_s[...] = jnp.zeros_like(both_s)

    def expert(e, carry):
        at = lane + e * slots
        pick = jnp.concatenate([(at == q[:, k : k + 1]).astype(jnp.bfloat16) for k in range(2)], axis=0)
        both_s[...] += jnp.dot(pick, rows_ref[e], preferred_element_type=jnp.float32)
        return carry

    lax.fori_loop(0, experts, expert, 0)
    mixed = gate_ref[:, 0:1] * both_s[:toks, :] + gate_ref[:, 1:2] * both_s[toks:, :]
    out_ref[...] = (x_ref[...].astype(jnp.float32) + mixed).astype(out_ref.dtype)


def mix_piece(toks, at, rows, tokens, slot, gate):
    experts, slots, cols = rows.shape
    blk = 64
    return pl.pallas_call(
        mix_kernel,
        grid_spec=pltpu.PrefetchScalarGridSpec(
            num_scalar_prefetch=1,
            grid=(toks // blk,),
            in_specs=[
                pl.BlockSpec((experts, slots, cols), lambda i, at: (0, 0, 0)),
                pl.BlockSpec((blk, cols), lambda i, at: (at[1] * (toks // blk) + i, at[0])),
                pl.BlockSpec((blk, 2), lambda i, at: (i, 0)),
                pl.BlockSpec((blk, LANES), lambda i, at: (at[1] * (toks // blk) + i, 0)),
            ],
            out_specs=pl.BlockSpec((blk, cols), lambda i, at: (i, 0)),
            scratch_shapes=[pltpu.VMEM((2 * blk, cols), jnp.float32)],
        ),
        out_shape=jax.ShapeDtypeStruct((toks, cols), tokens.dtype),
        compiler_params=pltpu.CompilerParams(vmem_limit_bytes=40 * 1024 * 1024),
        cost_estimate=pl.CostEstimate(flops=4 * toks * rows.size, bytes_accessed=2 * (rows.size + 2 * toks * cols), transcendentals=0),
        name="mix",
    )(at, rows, tokens, slot, gate)


def mix_share_kernel(peers, homes, count, *refs):
    rows_refs, away_ref = refs[: count - 1], refs[count - 1]
    slot_ref, gate_ref, x_ref, out_ref, x_s, o_s, rows_s = refs[count : count + 7]
    rows_sem, x_sem, own_sem, send_sem, recv_sem, pass_sem, passed_sem, stay_sem, go_sem, come_sem = refs[count + 7 :]
    toks, cols = o_s.shape
    blk = SHARE
    blocks = toks // blk
    me, here_e = lax.axis_index("tp"), lax.axis_index("ep")
    sides = (lax.rem(me + 1, peers), lax.rem(me + peers - 1, peers))

    def columns(owner):
        return pl.ds(pl.multiple_of(owner * cols, cols), cols)

    fetch = pltpu.make_async_copy(x_ref.at[:, columns(me)], x_s, x_sem)
    fetch.start()
    loads = [pltpu.make_async_copy(ref, rows_s.at[n], rows_sem.at[n]) for n, ref in enumerate(rows_refs)]
    for load in loads:
        load.start()
    barrier = pltpu.get_barrier_semaphore()
    for side in sides:
        pl.semaphore_signal(barrier, inc=1, device_id={"tp": side}, device_id_type=pl.DeviceIdType.MESH)
    for r in range(1, homes):
        other = lax.rem(here_e + r, homes)
        pl.semaphore_signal(barrier, inc=1, device_id={"ep": other}, device_id_type=pl.DeviceIdType.MESH)
    pl.semaphore_wait(barrier, homes + 1)

    slots = away_ref.shape[1]
    mine_e = pl.ds(pl.multiple_of(here_e * slots, ALIGN), slots)
    stay = pltpu.make_async_copy(away_ref.at[here_e], rows_s.at[count - 1, mine_e], stay_sem)
    stay.start()
    trips = []
    for r in range(1, homes):
        other = lax.rem(here_e + r, homes)
        trips.append(
            pltpu.make_async_remote_copy(
                src_ref=away_ref.at[other], dst_ref=rows_s.at[count - 1, mine_e],
                send_sem=go_sem.at[r - 1], recv_sem=come_sem.at[r - 1],
                device_id={"ep": other}, device_id_type=pl.DeviceIdType.MESH,
            )
        )
        trips[-1].start()
    fetch.wait()
    for load in loads:
        load.wait()

    def own(b):
        here = pl.ds(pl.multiple_of(b * blk, blk), blk)
        return pltpu.make_async_copy(o_s.at[here], out_ref.at[here, columns(me)], own_sem.at[b])

    def send(k, b):
        here = pl.ds(pl.multiple_of(b * blk, blk), blk)
        return pltpu.make_async_remote_copy(
            src_ref=o_s.at[here], dst_ref=out_ref.at[here, columns(me)],
            send_sem=send_sem.at[k, b], recv_sem=recv_sem.at[k, b],
            device_id={"tp": sides[k]}, device_id_type=pl.DeviceIdType.MESH,
        )

    def hand_on(k, b):
        half = pl.ds(pl.multiple_of(b * blk + k * (blk // 2), blk // 2), blk // 2)
        part = out_ref.at[half, columns(sides[1 - k])]
        return pltpu.make_async_remote_copy(
            src_ref=part, dst_ref=part,
            send_sem=pass_sem.at[k, b], recv_sem=passed_sem.at[k, b],
            device_id={"tp": sides[k]}, device_id_type=pl.DeviceIdType.MESH,
        )

    def relay(b):
        for k in range(2):
            send(k, b).wait_recv()
            hand_on(k, b).start()

    steps = blocks // count
    lane = lax.broadcasted_iota(jnp.int32, (blk, rows_s.shape[1]), 1)

    def block(b, carry):
        here = pl.ds(pl.multiple_of(b * blk, blk), blk)

        @pl.when(b == blocks - steps)
        def _():
            stay.wait()
            for trip in trips:
                trip.wait()

        q = slot_ref[here, :]
        gate = gate_ref[here, :]
        mixed = jnp.zeros((blk, cols), jnp.float32)
        for k in range(2):
            pick = (lane == q[:, k : k + 1]).astype(jnp.bfloat16)
            mixed += gate[:, k : k + 1] * jnp.dot(pick, rows_s[b // steps], preferred_element_type=jnp.float32)
        o_s[here, :] = (x_s[here, :].astype(jnp.float32) + mixed).astype(o_s.dtype)
        own(b).start()
        for k in range(2):
            send(k, b).start()

        @pl.when(b > 0)
        def _():
            relay(b - 1)

        return carry

    lax.fori_loop(0, blocks, block, 0)
    relay(blocks - 1)

    def finish(b, carry):
        own(b).wait()
        for k in range(2):
            send(k, b).wait_send()
            hand_on(k, b).wait()
        return carry

    lax.fori_loop(0, blocks, finish, 0)


def mix_share(peers, rows, away, tokens, slot, gate, name_id):
    assert peers == 4 and len(set(PIECES)) == 1
    homes, _, cols = away.shape
    toks = tokens.shape[0]
    blocks = toks // SHARE
    count = len(rows) + 1
    vmem, hbm = pl.BlockSpec(memory_space=pltpu.VMEM), pl.BlockSpec(memory_space=pl.ANY)
    return pl.pallas_call(
        functools.partial(mix_share_kernel, peers, homes, count),
        in_specs=[hbm] * count + [vmem, vmem, hbm],
        out_specs=hbm,
        out_shape=pltpu.HBM(tokens.shape, tokens.dtype),
        scratch_shapes=[
            pltpu.VMEM((toks, cols), tokens.dtype),
            pltpu.VMEM((toks, cols), tokens.dtype),
            pltpu.VMEM((count, homes * away.shape[1], cols), away.dtype),
            pltpu.SemaphoreType.DMA((count - 1,)),
            pltpu.SemaphoreType.DMA,
            pltpu.SemaphoreType.DMA((blocks,)),
        ]
        + [pltpu.SemaphoreType.DMA((2, blocks))] * 4
        + [pltpu.SemaphoreType.DMA, pltpu.SemaphoreType.DMA((homes - 1,)), pltpu.SemaphoreType.DMA((homes - 1,))],
        compiler_params=pltpu.CompilerParams(
            collective_id=name_id, has_side_effects=True, vmem_limit_bytes=40 * 1024 * 1024
        ),
        cost_estimate=pl.CostEstimate(flops=4 * toks * away.size, bytes_accessed=16 * toks * cols, transcendentals=0),
    )(*rows, pltpu.with_memory_space_constraint(away, pltpu.HBM), slot, gate, tokens)


def tell_kernel(homes, ids_ref, all_ref, own_sem, send_sem, recv_sem):
    me = lax.axis_index("ep")
    others = [lax.rem(me + r, homes) for r in range(1, homes)]
    barrier = pltpu.get_barrier_semaphore()
    for other in others:
        pl.semaphore_signal(barrier, inc=1, device_id={"ep": other}, device_id_type=pl.DeviceIdType.MESH)
    pl.semaphore_wait(barrier, homes - 1)
    copies = [pltpu.make_async_copy(ids_ref, all_ref.at[me], own_sem)]
    for r, other in enumerate(others):
        copies.append(
            pltpu.make_async_remote_copy(
                src_ref=ids_ref, dst_ref=all_ref.at[me], send_sem=send_sem.at[r], recv_sem=recv_sem.at[r],
                device_id={"ep": other}, device_id_type=pl.DeviceIdType.MESH,
            )
        )
    for copy in copies:
        copy.start()
    for copy in copies:
        copy.wait()


def tell_ids(homes, ids, name_id):
    anyspec = pl.BlockSpec(memory_space=pl.ANY)
    dma = pltpu.SemaphoreType.DMA
    return pl.pallas_call(
        functools.partial(tell_kernel, homes),
        in_specs=[anyspec],
        out_specs=anyspec,
        out_shape=pltpu.HBM((homes, *ids.shape), ids.dtype),
        scratch_shapes=[dma, dma((homes - 1,)), dma((homes - 1,))],
        compiler_params=pltpu.CompilerParams(collective_id=name_id, has_side_effects=True),
        cost_estimate=pl.CostEstimate(flops=1 << 20, bytes_accessed=2 * homes * ids.size * 4, transcendentals=0),
        name="tell",
    )(pltpu.with_memory_space_constraint(ids, pltpu.HBM))


def unwritten(like):
    return pl.pallas_call(
        lambda out_ref: None,
        out_specs=pl.BlockSpec(memory_space=pl.ANY),
        out_shape=pltpu.HBM(like.shape, like.dtype),
        name="unwritten",
    )()


def after(x, *earlier):
    return lax.optimization_barrier((x, *earlier))[0]


def solution(mesh):
    tp, ep = mesh.shape["tp"], mesh.shape["ep"]
    tok_spec = P(("dp", "ep"), None)

    def local_block(tokens, ids, gain, router_w, w_gate, w_up, w_down):
        num_tok, dim = tokens.shape
        num_exp = router_w.shape[1]
        assert num_exp == ep and ids.shape[1] == 2
        assert sum(PIECES) == num_tok
        begin = [sum(PIECES[:p]) for p in range(len(PIECES))]
        gain2 = gain.reshape(1, dim)
        rw = jnp.pad(router_w, ((0, 0), (0, LANES - num_exp)))
        me, col = lax.axis_index("ep"), lax.axis_index("tp")
        cols = dim // tp

        home = [(g, sum(sizes[:i])) for g, (sizes, _) in enumerate(GROUPS) for i in range(len(sizes))]
        group_begin = [begin[[h[0] for h in home].index(g)] for g in range(len(GROUPS))]

        def norm_group(g):
            size, wide = sum(GROUPS[g][0]), GROUPS[g][1]
            if wide:
                return norm_rows(group_begin[g], size // tp, col.reshape(1), tokens, gain2, 128)
            return norm_rows(group_begin[g], size, jnp.zeros((1,), jnp.int32), tokens, gain2)

        def gather_group(g, h):
            return lax.all_gather(h, ("ep", "tp") if GROUPS[g][1] else "ep", axis=0, tiled=True)

        normed = [norm_group(g) for g in range(len(GROUPS))]
        hall0 = gather_group(0, normed[0])
        gates = gate_rows(tokens, ids, gain2, rw)

        w13, w2 = pair_columns(w_gate[0], w_up[0]), block_columns(w_down[0])

        ids_t = ids.T
        all_ids = tell_ids(ep, ids_t, len(LEVELS))
        experts = jnp.arange(num_exp, dtype=jnp.int32)
        earlier = jnp.arange(ep)[None, :] < jnp.arange(ep)[:, None]
        most_rows, most_slots = [], []
        positions, fast_meta, full_meta, fast_rows, full_rows = [], [], [], [], []
        for p, (b, n) in enumerate(zip(begin, PIECES)):
            before = (jnp.arange(n)[:, None] < jnp.arange(n)[None, :]).astype(jnp.bfloat16)

            def rank(mask):
                return jnp.dot(mask.astype(jnp.bfloat16), before, preferred_element_type=jnp.float32).astype(jnp.int32)

            piece = all_ids[:, :, b : b + n]
            hit = (piece[None] == experts[:, None, None, None]).any(axis=2)
            load = jnp.sum(hit.astype(jnp.int32), axis=-1)
            padded = (load + ALIGN - 1) // ALIGN * ALIGN
            most_rows.append(jnp.max(jnp.sum(padded, axis=1)))
            most_slots.append(jnp.max(load))

            mine = (piece == me).any(axis=1)
            my_pad = (jnp.sum(mine.astype(jnp.int32), axis=-1) + ALIGN - 1) // ALIGN * ALIGN
            base = jnp.sum(jnp.where(earlier, my_pad[None, :], 0), axis=-1)
            pos = base[:, None] + rank(mine)
            starts = pos[:, ::CHUNK].reshape(-1) // ALIGN * ALIGN
            pos = jnp.where(mine, pos, -1).reshape(ep * n // CHUNK, 1, CHUNK)

            def limits(cap, slots, *tilings):
                tile_rows = tilings[min(p, len(tilings) - 1)][0]
                tiles = jnp.minimum((jnp.sum(my_pad) + tile_rows - 1) // tile_rows, cap // tile_rows)
                at = jnp.concatenate([jnp.minimum(starts, cap), tiles[None]])
                count = jnp.minimum(jnp.minimum(my_pad, slots), jnp.maximum(cap - base, 0)) // ALIGN
                return at.astype(jnp.int32), jnp.concatenate([base, count]).astype(jnp.int32)

            positions.append(pos)
            fast_meta.append([limits(*room) for room in LEVELS])
            full_meta.append(limits(ep * n, n, (SPARE_TILE,)))

            own = ids_t[:, b : b + n]
            own_hit = own[None] == experts[:, None, None]
            own_rank = rank(own_hit.any(axis=1))
            own_slot = jnp.sum(jnp.where(own_hit, own_rank[:, None], 0), axis=0)
            fast_rows.append([(own * level[1] + own_slot).T for level in LEVELS])
            full_rows.append((own * n + own_slot).T)

        def reduce(y):
            return lax.psum_scatter(y, "tp", scatter_dimension=1, tiled=True)

        def swap(y):
            return lax.all_to_all(y, "ep", 0, 0, tiled=True)

        def spare(hall0):
            n = PIECES[0]
            stacked = jax.tree.map(lambda *a: jnp.stack(a), *zip(full_meta, positions, full_rows))

            def body(p, out):
                (meta, spread_meta), pos, own_row = jax.tree.map(lambda a: lax.dynamic_index_in_dim(a, p, 0, False), stacked)
                h = norm_rows(0, n, p.reshape(1), tokens, gain2)
                hall = lax.all_gather(h, "ep", axis=0, tiled=True)
                y = reduce(ffn_piece(1, ep * n, SPARE_TILE, (n, 0), n // CHUNK, meta, pos, hall, w13, w2))
                y = swap(spread_piece(n, ep, spread_meta, y).reshape(ep, n, cols))
                o = mix_piece(n, jnp.stack([col, p]), y, tokens, own_row, gates)
                o = lax.all_gather(o, "tp", axis=1, tiled=True)
                return lax.dynamic_update_slice_in_dim(out, o, p * n, 0)

            return lax.fori_loop(0, len(PIECES), body, unwritten(tokens))

        def fast(level, hall0):
            cap, slots, *tilings = LEVELS[level]
            last, halls, reds, backs = None, {0: hall0}, {}, {}
            for step in ORDER:
                kind, names = step[0], [int(c) for c in step[1:]]
                p = names[0]
                if kind == "A":
                    halls[p] = gather_group(p, normed[p] if last is None else after(normed[p], last))
                elif kind == "F":
                    g, at = home[p]
                    hall = halls[g] if last is None else after(halls[g], last)
                    rows_of, per_block = (sum(GROUPS[g][0]), at), PIECES[p] // CHUNK
                    tile_rows, unroll = tilings[min(p, 1)]
                    last = ffn_piece(unroll, cap, tile_rows, rows_of, per_block, fast_meta[p][level][0], positions[p], hall, w13, w2)
                    reds[p] = reduce(last)
                elif kind == "S":
                    last = spread_piece(slots, ep, fast_meta[p][level][1], after(reds[p], last))
                    backs[p] = last.reshape(ep, slots, cols)
                    if p < len(PIECES) - 1:
                        backs[p] = swap(backs[p])
                else:
                    rows = [after(backs[q], last).reshape(-1, cols) for q in names[:-1]]
                    own_rows = jnp.concatenate([fast_rows[q][level] for q in names])
                    out = mix_share(tp, rows, backs[names[-1]], tokens, own_rows, gates, level)
            return out

        need = jnp.int32(0)
        for i, (cap, slots, *_) in enumerate(LEVELS):
            over = (functools.reduce(jnp.maximum, most_rows) > cap) | (functools.reduce(jnp.maximum, most_slots) > slots)
            need = jnp.where(over, i + 1, need)
        if mesh.shape["dp"] > 1:
            need = lax.pmax(need, "dp")
        paths = [functools.partial(fast, i) for i in range(len(LEVELS))]
        return lax.switch(need, [*paths, spare], hall0)

    return jax.shard_map(
        local_block,
        mesh=mesh,
        in_specs=(tok_spec, tok_spec, P(None), P(None, None), P("ep", None, "tp"), P("ep", None, "tp"), P("ep", "tp", None)),
        out_specs=tok_spec,
        check_vma=False,
    )
```

```python
import functools

import jax
import jax.numpy as jnp
from jax import lax
from jax.experimental import pallas as pl
from jax.experimental.pallas import tpu as pltpu
from jax.sharding import PartitionSpec as P


NORM_EPS = 1e-5
GROUPS = (((512, 512), True), ((512,), False), ((512,), False))
PIECES = sum((sizes for sizes, _ in GROUPS), ())
CHUNK = 256
ALIGN = 16
WIN = CHUNK + ALIGN
SHARE = 128
ORDER = ("A1", "A2", "F0", "F1", "F2", "S0", "S1", "F3", "S2", "S3", "M0")
TRIPS = ((0, 1), (2,), (3,))
LEVELS = ((1472, 320, (128, True), (192, 2)), (1792, 320, (256, 2), (256, 1)))
SPARE_TILE = 128
LANES = 128


def rms_norm(x_ref, gain_ref):
    x = x_ref[...].astype(jnp.float32)
    inv = lax.rsqrt(jnp.mean(x * x, axis=-1, keepdims=True) + NORM_EPS)
    return (x * inv * gain_ref[...].astype(jnp.float32)).astype(jnp.bfloat16)


def norm_kernel(at_ref, x_ref, gain_ref, h_ref):
    h_ref[...] = rms_norm(x_ref, gain_ref)


def norm_rows(begin, rows, share, tokens, gain, blk=64):
    dim = tokens.shape[1]
    return pl.pallas_call(
        norm_kernel,
        grid_spec=pltpu.PrefetchScalarGridSpec(
            num_scalar_prefetch=1,
            grid=(rows // blk,),
            in_specs=[
                pl.BlockSpec((blk, dim), lambda i, at: (begin // blk + at[0] * (rows // blk) + i, 0)),
                pl.BlockSpec((1, dim), lambda i, at: (0, 0)),
            ],
            out_specs=pl.BlockSpec((blk, dim), lambda i, at: (i, 0)),
        ),
        out_shape=pltpu.HBM((rows, dim), jnp.bfloat16),
        cost_estimate=pl.CostEstimate(flops=8 * rows * dim, bytes_accessed=4 * rows * dim, transcendentals=0),
        name="norm",
    )(share, tokens, gain)


def gate_kernel(x_ref, ids_ref, gain_ref, rw_ref, gate_ref):
    logits = jnp.dot(rms_norm(x_ref, gain_ref), rw_ref[...], preferred_element_type=jnp.float32)
    lane = lax.broadcasted_iota(jnp.int32, logits.shape, 1)
    ids = ids_ref[...]
    l0 = jnp.sum(jnp.where(lane == ids[:, 0:1], logits, 0.0), axis=-1, keepdims=True)
    l1 = jnp.sum(jnp.where(lane == ids[:, 1:2], logits, 0.0), axis=-1, keepdims=True)
    top = jnp.maximum(l0, l1)
    e0, e1 = jnp.exp(l0 - top), jnp.exp(l1 - top)
    tot = e0 + e1
    gate_ref[...] = jnp.where(lane == 0, e0 / tot, jnp.where(lane == 1, e1 / tot, 0.0))


def gate_rows(tokens, ids, gain, rw):
    rows, dim = tokens.shape
    blk = 64
    return pl.pallas_call(
        gate_kernel,
        grid=(rows // blk,),
        in_specs=[
            pl.BlockSpec((blk, dim), lambda i: (i, 0)),
            pl.BlockSpec((blk, ids.shape[1]), lambda i: (i, 0)),
            pl.BlockSpec((1, dim), lambda i: (0, 0)),
            pl.BlockSpec((dim, LANES), lambda i: (0, 0)),
        ],
        out_specs=pl.BlockSpec((blk, LANES), lambda i: (i, 0)),
        out_shape=jax.ShapeDtypeStruct((rows, LANES), jnp.float32),
        cost_estimate=pl.CostEstimate(flops=2 * rows * dim * LANES, bytes_accessed=2 * rows * dim, transcendentals=0),
        name="gate",
    )(tokens, ids, gain, rw)


def ffn_kernel(unroll, tile_rows, rows_of, per_block, meta_ref, pos_ref, hall_ref, w13_hbm, w2_hbm, y_ref,
               w13_ref, w2_ref, rows_s, u_s, hbuf, obuf, wsem, hsem, osem):
    chunks = pos_ref.shape[0]
    nup, _, pair = w13_ref.shape
    half = pair // 2
    ndown, _, wide = w2_ref.shape
    slots = hbuf.shape[0]

    def fetch(j):
        slot = lax.rem(j, slots)
        row = pl.multiple_of((j // per_block) * rows_of[0] + rows_of[1] + lax.rem(j, per_block) * CHUNK, CHUNK)
        return pltpu.make_async_copy(hall_ref.at[pl.ds(row, CHUNK)], hbuf.at[slot], hsem.at[slot])

    for j in range(slots - 1):
        fetch(j).start()
    weights = [pltpu.make_async_copy(w13_hbm, w13_ref, wsem.at[0]), pltpu.make_async_copy(w2_hbm, w2_ref, wsem.at[1])]
    for w in weights:
        w.start()

    def compact(j, carry):
        @pl.when(j + slots - 1 < chunks)
        def _():
            fetch(j + slots - 1).start()

        fetch(j).wait()
        slot = lax.rem(j, slots)
        start = pl.multiple_of(meta_ref[j], ALIGN)
        rel = pos_ref[j] - start
        pick = (lax.broadcasted_iota(jnp.int32, (WIN, CHUNK), 0) == rel).astype(jnp.bfloat16)
        got = jnp.dot(pick, hbuf[slot], preferred_element_type=jnp.float32).astype(jnp.bfloat16)
        old = rows_s[pl.ds(start, ALIGN), :]
        old = jnp.where(j == 0, jnp.zeros_like(old), old)
        rows_s[pl.ds(start, ALIGN), :] = old + got[:ALIGN]
        rows_s[pl.ds(start + ALIGN, CHUNK), :] = got[ALIGN:]
        return carry

    lax.fori_loop(0, chunks, compact, 0)
    for w in weights:
        w.wait()

    full, rest = divmod(y_ref.shape[0], tile_rows)

    def put(i, act):
        slot = lax.rem(i, 2)

        def copy(rows):
            at = pl.ds(pl.multiple_of(i * tile_rows, ALIGN), rows)
            return pltpu.make_async_copy(obuf.at[slot, pl.ds(0, rows)], y_ref.at[at], osem.at[slot])

        @pl.when(i < full)
        def _():
            act(copy(tile_rows))

        if rest:

            @pl.when(i >= full)
            def _():
                act(copy(rest))

    tiles = meta_ref[chunks]

    def tile(i, carry):
        slot = lax.rem(i, 2)
        a = rows_s[pl.ds(pl.multiple_of(i * tile_rows, ALIGN), tile_rows), :]

        def up_step(j, c):
            both = jnp.dot(a, w13_ref[j], preferred_element_type=jnp.float32)
            act, up = both[:, :half], both[:, half:]
            u_s[:, pl.ds(pl.multiple_of(j * half, half), half)] = (jax.nn.silu(act) * up).astype(jnp.bfloat16)
            return c

        lax.fori_loop(0, nup, up_step, 0, unroll=unroll)

        @pl.when(i >= 2)
        def _():
            put(i - 2, lambda c: c.wait())

        u = u_s[...]

        def down_step(j, c):
            obuf[slot, :, pl.ds(pl.multiple_of(j * wide, wide), wide)] = jnp.dot(
                u, w2_ref[j], preferred_element_type=jnp.float32
            ).astype(jnp.bfloat16)
            return c

        lax.fori_loop(0, ndown, down_step, 0, unroll=unroll)
        put(i, lambda c: c.start())
        return carry

    lax.fori_loop(0, tiles, tile, 0)

    @pl.when(tiles >= 2)
    def _():
        put(tiles - 2, lambda c: c.wait())

    @pl.when(tiles >= 1)
    def _():
        put(tiles - 1, lambda c: c.wait())


def ffn_piece(unroll, cap, tile_rows, rows_of, per_block, meta, pos, hall, w13, w2):
    dim, width = w13.shape[1], w2.shape[1]
    slots = 4
    hbm = pl.BlockSpec(memory_space=pltpu.HBM)
    vmem = pl.BlockSpec(memory_space=pltpu.VMEM)
    scratch = 2 * dim * (cap + WIN + slots * CHUNK + 2 * tile_rows) + 2 * tile_rows * width
    return pl.pallas_call(
        functools.partial(ffn_kernel, unroll, tile_rows, rows_of, per_block),
        in_specs=[pl.BlockSpec(memory_space=pltpu.SMEM), vmem, hbm, hbm, hbm],
        out_specs=hbm,
        scratch_shapes=[
            pltpu.VMEM(w13.shape, w13.dtype),
            pltpu.VMEM(w2.shape, w2.dtype),
            pltpu.VMEM((cap + WIN, dim), jnp.bfloat16),
            pltpu.VMEM((tile_rows, width), jnp.bfloat16),
            pltpu.VMEM((slots, CHUNK, dim), jnp.bfloat16),
            pltpu.VMEM((2, tile_rows, dim), jnp.bfloat16),
            pltpu.SemaphoreType.DMA((2,)),
            pltpu.SemaphoreType.DMA((slots,)),
            pltpu.SemaphoreType.DMA((2,)),
        ],
        out_shape=pltpu.HBM((cap, dim), jnp.bfloat16),
        compiler_params=pltpu.CompilerParams(vmem_limit_bytes=scratch + 2 * (w13.size + w2.size) + 6 * 1024 * 1024),
        cost_estimate=pl.CostEstimate(
            flops=6 * (cap * 3 // 4) * dim * width, bytes_accessed=2 * (hall.size + cap * dim), transcendentals=0
        ),
        name="ffn",
    )(meta, pos, *(pltpu.with_memory_space_constraint(a, pltpu.HBM) for a in (hall, w13, w2)))


def pair_kernel(w1_ref, w3_ref, out_ref):
    half = w1_ref.shape[1]
    out_ref[0, :, :half] = w1_ref[...]
    out_ref[0, :, half:] = w3_ref[...]


def pair_columns(w1, w3):
    dim, width = w1.shape
    return pl.pallas_call(
        pair_kernel,
        grid=(width // LANES,),
        in_specs=[pl.BlockSpec((dim, LANES), lambda j: (0, j))] * 2,
        out_specs=pl.BlockSpec((1, dim, 2 * LANES), lambda j: (j, 0, 0)),
        out_shape=pltpu.HBM((width // LANES, dim, 2 * LANES), w1.dtype),
        cost_estimate=pl.CostEstimate(flops=8 * dim * width, bytes_accessed=8 * dim * width, transcendentals=0),
        name="pair",
    )(w1, w3)


def block_kernel(w_ref, out_ref):
    out_ref[0] = w_ref[...]


def block_columns(w):
    width, dim = w.shape
    wide = 2 * LANES
    return pl.pallas_call(
        block_kernel,
        grid=(dim // wide,),
        in_specs=[pl.BlockSpec((width, wide), lambda j: (0, j))],
        out_specs=pl.BlockSpec((1, width, wide), lambda j: (j, 0, 0)),
        out_shape=pltpu.HBM((dim // wide, width, wide), w.dtype),
        cost_estimate=pl.CostEstimate(flops=4 * dim * width, bytes_accessed=4 * dim * width, transcendentals=0),
        name="block",
    )(w)


def spread_kernel(part, meta_ref, y_ref, *refs):
    out_ref, lay_s, sem = refs[-3:]
    blocks, slots, cols = lay_s.shape

    def block(s, carry):
        def clear(g, carry):
            lay_s[s, pl.ds(pl.multiple_of(g * ALIGN, ALIGN), ALIGN), :] = jnp.zeros((ALIGN, cols), lay_s.dtype)
            return carry

        def move(g, carry):
            src = pl.multiple_of(meta_ref[s] + g * ALIGN, ALIGN)
            lay_s[s, pl.ds(pl.multiple_of(g * ALIGN, ALIGN), ALIGN), :] = y_ref[pl.ds(src, ALIGN), :]
            return carry

        runs = meta_ref[blocks + s]
        lax.fori_loop(0, runs, move, 0)
        lax.fori_loop(runs, slots // ALIGN, clear, 0)
        return carry

    lax.fori_loop(0, blocks, block, 0)
    copy = pltpu.make_async_copy(lay_s, out_ref.at[:, pl.ds(part * slots, slots)], sem)
    copy.start()
    copy.wait()


def spread_piece(slots, blocks, meta, y, part=0, parts=1, earlier=None):
    cap, cols = y.shape
    hbm = pl.BlockSpec(memory_space=pl.ANY)
    more = [] if earlier is None else [pltpu.with_memory_space_constraint(earlier, pltpu.HBM)]
    return pl.pallas_call(
        functools.partial(spread_kernel, part),
        in_specs=[pl.BlockSpec(memory_space=pltpu.SMEM), pl.BlockSpec(memory_space=pltpu.VMEM)] + [hbm] * len(more),
        out_specs=hbm,
        out_shape=pltpu.HBM((blocks, parts * slots, cols), y.dtype),
        scratch_shapes=[pltpu.VMEM((blocks, slots, cols), y.dtype), pltpu.SemaphoreType.DMA],
        input_output_aliases={2: 0} if more else {},
        cost_estimate=pl.CostEstimate(flops=1 << 20, bytes_accessed=4 * (cap + blocks * slots) * cols, transcendentals=0),
        name="spread",
    )(meta, y, *more)


def mix_kernel(col_ref, rows_ref, x_ref, slot_ref, gate_ref, out_ref, both_s):
    toks = x_ref.shape[0]
    experts, slots, _ = rows_ref.shape
    lane = lax.broadcasted_iota(jnp.int32, (toks, slots), 1)
    q = slot_ref[...]
    both_s[...] = jnp.zeros_like(both_s)

    def expert(e, carry):
        at = lane + e * slots
        pick = jnp.concatenate([(at == q[:, k : k + 1]).astype(jnp.bfloat16) for k in range(2)], axis=0)
        both_s[...] += jnp.dot(pick, rows_ref[e], preferred_element_type=jnp.float32)
        return carry

    lax.fori_loop(0, experts, expert, 0)
    mixed = gate_ref[:, 0:1] * both_s[:toks, :] + gate_ref[:, 1:2] * both_s[toks:, :]
    out_ref[...] = (x_ref[...].astype(jnp.float32) + mixed).astype(out_ref.dtype)


def mix_piece(toks, at, rows, tokens, slot, gate):
    experts, slots, cols = rows.shape
    blk = 64
    return pl.pallas_call(
        mix_kernel,
        grid_spec=pltpu.PrefetchScalarGridSpec(
            num_scalar_prefetch=1,
            grid=(toks // blk,),
            in_specs=[
                pl.BlockSpec((experts, slots, cols), lambda i, at: (0, 0, 0)),
                pl.BlockSpec((blk, cols), lambda i, at: (at[1] * (toks // blk) + i, at[0])),
                pl.BlockSpec((blk, 2), lambda i, at: (i, 0)),
                pl.BlockSpec((blk, LANES), lambda i, at: (at[1] * (toks // blk) + i, 0)),
            ],
            out_specs=pl.BlockSpec((blk, cols), lambda i, at: (i, 0)),
            scratch_shapes=[pltpu.VMEM((2 * blk, cols), jnp.float32)],
        ),
        out_shape=jax.ShapeDtypeStruct((toks, cols), tokens.dtype),
        compiler_params=pltpu.CompilerParams(vmem_limit_bytes=40 * 1024 * 1024),
        cost_estimate=pl.CostEstimate(flops=4 * toks * rows.size, bytes_accessed=2 * (rows.size + 2 * toks * cols), transcendentals=0),
        name="mix",
    )(at, rows, tokens, slot, gate)


def mix_share_kernel(peers, homes, places, *refs):
    count, arrays = len(places) + 1, places[-1][0] + 1
    rows_refs, away_ref = refs[:arrays], refs[arrays]
    slot_ref, gate_ref, x_ref, out_ref, x_s, rows_s = refs[arrays + 1 : arrays + 7]
    rows_sem, x_sem, stay_sem, send_sem, recv_sem, pass_sem, passed_sem, go_sem, come_sem = refs[arrays + 7 :]
    toks, cols = x_s.shape
    blk = SHARE
    blocks = toks // blk
    steps = blocks // count
    slots = away_ref.shape[1]
    me, here_e = lax.axis_index("tp"), lax.axis_index("ep")
    sides = (lax.rem(me + 1, peers), lax.rem(me + peers - 1, peers))

    def columns(owner):
        return pl.ds(pl.multiple_of(owner * cols, cols), cols)

    loads = [
        pltpu.make_async_copy(x_ref.at[:, columns(me)], x_s, x_sem),
        pltpu.make_async_copy(away_ref.at[here_e], rows_s.at[count - 1, here_e], stay_sem),
        *(
            pltpu.make_async_copy(rows_refs[i].at[:, pl.ds(q * slots, slots)], rows_s.at[n], rows_sem.at[n])
            for n, (i, q) in enumerate(places)
        ),
    ]
    for load in loads:
        load.start()
    barrier = pltpu.get_barrier_semaphore()
    for side in sides:
        pl.semaphore_signal(barrier, inc=1, device_id={"tp": side}, device_id_type=pl.DeviceIdType.MESH)
    for r in range(1, homes):
        other = lax.rem(here_e + r, homes)
        pl.semaphore_signal(barrier, inc=1, device_id={"ep": other}, device_id_type=pl.DeviceIdType.MESH)
    pl.semaphore_wait(barrier, homes + 1)

    def trip(r):
        other = lax.rem(here_e + r, homes)
        return pltpu.make_async_remote_copy(
            src_ref=away_ref.at[other], dst_ref=rows_s.at[count - 1, here_e],
            send_sem=go_sem.at[r - 1], recv_sem=come_sem.at[r - 1],
            device_id={"ep": other}, device_id_type=pl.DeviceIdType.MESH,
        )

    for r in range(1, homes):
        trip(r).start()
    loads[0].wait()

    def send(k, b):
        mine = out_ref.at[pl.ds(pl.multiple_of(b * blk, blk), blk), columns(me)]
        return pltpu.make_async_remote_copy(
            src_ref=mine, dst_ref=mine, send_sem=send_sem.at[k, b], recv_sem=recv_sem.at[k, b],
            device_id={"tp": sides[k]}, device_id_type=pl.DeviceIdType.MESH,
        )

    def hand_on(k, b):
        half = out_ref.at[pl.ds(pl.multiple_of(b * blk + k * (blk // 2), blk // 2), blk // 2), columns(sides[1 - k])]
        return pltpu.make_async_remote_copy(
            src_ref=half, dst_ref=half, send_sem=pass_sem.at[k, b], recv_sem=passed_sem.at[k, b],
            device_id={"tp": sides[k]}, device_id_type=pl.DeviceIdType.MESH,
        )

    def relay(b):
        for k in range(2):
            send(k, b).wait_recv()
            hand_on(k, b).start()

    lane = lax.broadcasted_iota(jnp.int32, (blk, homes * slots), 1)

    def block(b, carry):
        here = pl.ds(pl.multiple_of(b * blk, blk), blk)

        for n in range(count - 1):

            @pl.when(b == n * steps)
            def _(n=n):
                loads[2 + n].wait()

        @pl.when(b == blocks - steps)
        def _():
            loads[1].wait()
            for r in range(1, homes):
                trip(r).wait()

        q = slot_ref[here, :]
        gate = gate_ref[here, :]
        rows = rows_s[b // steps].reshape(homes * slots, cols)
        mixed = jnp.zeros((blk, cols), jnp.float32)
        for k in range(2):
            pick = (lane == q[:, k : k + 1]).astype(jnp.bfloat16)
            mixed += gate[:, k : k + 1] * jnp.dot(pick, rows, preferred_element_type=jnp.float32)
        out_ref[here, columns(me)] = (x_s[here, :].astype(jnp.float32) + mixed).astype(out_ref.dtype)
        for k in range(2):
            send(k, b).start()

        @pl.when(b > 0)
        def _():
            relay(b - 1)

        return carry

    lax.fori_loop(0, blocks, block, 0)
    relay(blocks - 1)

    def finish(b, carry):
        for k in range(2):
            send(k, b).wait_send()
            hand_on(k, b).wait()
        return carry

    lax.fori_loop(0, blocks, finish, 0)


def mix_share(peers, places, rows, away, tokens, slot, gate, name_id):
    assert peers == 4 and len(set(PIECES)) == 1
    homes, slots, cols = away.shape
    toks = tokens.shape[0]
    blocks = toks // SHARE
    count = len(places) + 1
    vmem, hbm = pl.BlockSpec(memory_space=pltpu.VMEM), pl.BlockSpec(memory_space=pl.ANY)
    dma = pltpu.SemaphoreType.DMA
    return pl.pallas_call(
        functools.partial(mix_share_kernel, peers, homes, places),
        in_specs=[hbm] * (len(rows) + 1) + [vmem, vmem, hbm],
        out_specs=vmem,
        out_shape=pltpu.VMEM(tokens.shape, tokens.dtype),
        scratch_shapes=[
            pltpu.VMEM((toks, cols), tokens.dtype),
            pltpu.VMEM((count, homes, slots, cols), tokens.dtype),
            dma((count - 1,)),
            dma,
            dma,
        ]
        + [dma((2, blocks))] * 4
        + [dma((homes - 1,)), dma((homes - 1,))],
        compiler_params=pltpu.CompilerParams(
            collective_id=name_id, has_side_effects=True, vmem_limit_bytes=36 * 1024 * 1024
        ),
        cost_estimate=pl.CostEstimate(flops=4 * toks * homes * slots * cols, bytes_accessed=16 * toks * cols, transcendentals=0),
    )(*rows, pltpu.with_memory_space_constraint(away, pltpu.HBM), slot, gate, tokens)


def settle_kernel(in_ref, out_ref, sem):
    copy = pltpu.make_async_copy(in_ref, out_ref, sem)
    copy.start()
    copy.wait()


def settle(x):
    return pl.pallas_call(
        settle_kernel,
        in_specs=[pl.BlockSpec(memory_space=pltpu.VMEM)],
        out_specs=pl.BlockSpec(memory_space=pl.ANY),
        out_shape=pltpu.HBM(x.shape, x.dtype),
        scratch_shapes=[pltpu.SemaphoreType.DMA],
        compiler_params=pltpu.CompilerParams(vmem_limit_bytes=1024 * 1024),
        cost_estimate=pl.CostEstimate(flops=x.size, bytes_accessed=4 * x.size, transcendentals=0),
        name="settle",
    )(pltpu.with_memory_space_constraint(x, pltpu.VMEM))


def tell_kernel(homes, ids_ref, all_ref, own_sem, send_sem, recv_sem):
    me = lax.axis_index("ep")
    others = [lax.rem(me + r, homes) for r in range(1, homes)]
    barrier = pltpu.get_barrier_semaphore()
    for other in others:
        pl.semaphore_signal(barrier, inc=1, device_id={"ep": other}, device_id_type=pl.DeviceIdType.MESH)
    pl.semaphore_wait(barrier, homes - 1)
    copies = [pltpu.make_async_copy(ids_ref, all_ref.at[me], own_sem)]
    for r, other in enumerate(others):
        copies.append(
            pltpu.make_async_remote_copy(
                src_ref=ids_ref, dst_ref=all_ref.at[me], send_sem=send_sem.at[r], recv_sem=recv_sem.at[r],
                device_id={"ep": other}, device_id_type=pl.DeviceIdType.MESH,
            )
        )
    for copy in copies:
        copy.start()
    for copy in copies:
        copy.wait()


def tell_ids(homes, ids, name_id):
    anyspec = pl.BlockSpec(memory_space=pl.ANY)
    dma = pltpu.SemaphoreType.DMA
    return pl.pallas_call(
        functools.partial(tell_kernel, homes),
        in_specs=[anyspec],
        out_specs=anyspec,
        out_shape=pltpu.HBM((homes, *ids.shape), ids.dtype),
        scratch_shapes=[dma, dma((homes - 1,)), dma((homes - 1,))],
        compiler_params=pltpu.CompilerParams(collective_id=name_id, has_side_effects=True),
        cost_estimate=pl.CostEstimate(flops=1 << 20, bytes_accessed=2 * homes * ids.size * 4, transcendentals=0),
        name="tell",
    )(pltpu.with_memory_space_constraint(ids, pltpu.HBM))


def unwritten(like):
    return pl.pallas_call(
        lambda out_ref: None,
        out_specs=pl.BlockSpec(memory_space=pl.ANY),
        out_shape=pltpu.HBM(like.shape, like.dtype),
        name="unwritten",
    )()


def after(x, *earlier):
    return lax.optimization_barrier((x, *earlier))[0]


def solution(mesh):
    tp, ep = mesh.shape["tp"], mesh.shape["ep"]
    tok_spec = P(("dp", "ep"), None)

    def local_block(tokens, ids, gain, router_w, w_gate, w_up, w_down):
        num_tok, dim = tokens.shape
        num_exp = router_w.shape[1]
        assert num_exp == ep and ids.shape[1] == 2
        assert sum(PIECES) == num_tok
        begin = [sum(PIECES[:p]) for p in range(len(PIECES))]
        gain2 = gain.reshape(1, dim)
        rw = jnp.pad(router_w, ((0, 0), (0, LANES - num_exp)))
        me, col = lax.axis_index("ep"), lax.axis_index("tp")

        home = [(g, sum(sizes[:i])) for g, (sizes, _) in enumerate(GROUPS) for i in range(len(sizes))]
        group_begin = [begin[[h[0] for h in home].index(g)] for g in range(len(GROUPS))]

        def norm_group(g):
            size, wide = sum(GROUPS[g][0]), GROUPS[g][1]
            if wide:
                return norm_rows(group_begin[g], size // tp, col.reshape(1), tokens, gain2, 128)
            return norm_rows(group_begin[g], size, jnp.zeros((1,), jnp.int32), tokens, gain2)

        def gather_group(g, h):
            return lax.all_gather(h, ("ep", "tp") if GROUPS[g][1] else "ep", axis=0, tiled=True)

        normed = [norm_group(g) for g in range(len(GROUPS))]
        hall0 = gather_group(0, normed[0])
        gates = gate_rows(tokens, ids, gain2, rw)

        w13, w2 = pair_columns(w_gate[0], w_up[0]), block_columns(w_down[0])

        ids_t = ids.T
        all_ids = tell_ids(ep, ids_t, len(LEVELS))
        experts = jnp.arange(num_exp, dtype=jnp.int32)
        earlier = jnp.arange(ep)[None, :] < jnp.arange(ep)[:, None]
        most_rows, most_slots = [], []
        positions, fast_meta, full_meta, fast_rows, full_rows = [], [], [], [], []
        for p, (b, n) in enumerate(zip(begin, PIECES)):
            before = (jnp.arange(n)[:, None] < jnp.arange(n)[None, :]).astype(jnp.bfloat16)

            def rank(mask):
                return jnp.dot(mask.astype(jnp.bfloat16), before, preferred_element_type=jnp.float32).astype(jnp.int32)

            piece = all_ids[:, :, b : b + n]
            hit = (piece[None] == experts[:, None, None, None]).any(axis=2)
            load = jnp.sum(hit.astype(jnp.int32), axis=-1)
            ahead = jnp.sum(jnp.where(earlier[None], load[:, None, :], 0), axis=-1)
            lean = ahead % ALIGN
            most_rows.append(jnp.max(jnp.sum(load, axis=1)))
            most_slots.append(jnp.max(lean + load))

            mine = (piece == me).any(axis=1)
            my_load = jnp.sum(mine.astype(jnp.int32), axis=-1)
            base = jnp.sum(jnp.where(earlier, my_load[None, :], 0), axis=-1)
            pos = base[:, None] + rank(mine)
            starts = pos[:, ::CHUNK].reshape(-1) // ALIGN * ALIGN
            pos = jnp.where(mine, pos, -1).reshape(ep * n // CHUNK, 1, CHUNK)

            def limits(cap, slots, *tilings):
                tile_rows = tilings[min(p, len(tilings) - 1)][0]
                tiles = jnp.minimum((jnp.sum(my_load) + tile_rows - 1) // tile_rows, -(-cap // tile_rows))
                at = jnp.concatenate([jnp.minimum(starts, cap), tiles[None]])
                src = base // ALIGN * ALIGN
                runs = jnp.minimum((base - src + my_load + ALIGN - 1) // ALIGN, slots // ALIGN)
                runs = jnp.minimum(runs, jnp.maximum(cap - src, 0) // ALIGN)
                return at.astype(jnp.int32), jnp.concatenate([src, runs]).astype(jnp.int32)

            positions.append(pos)
            fast_meta.append([limits(*room) for room in LEVELS])
            full_meta.append(limits(ep * n, n + ALIGN, (SPARE_TILE,)))

            own = ids_t[:, b : b + n]
            own_hit = own[None] == experts[:, None, None]
            my_lean = jnp.sum(jnp.where(jnp.arange(ep)[None, :] == me, lean, 0), axis=1)
            own_rank = rank(own_hit.any(axis=1)) + my_lean[:, None]
            own_slot = jnp.sum(jnp.where(own_hit, own_rank[:, None], 0), axis=0)
            fast_rows.append([(own * level[1] + own_slot).T for level in LEVELS])
            full_rows.append((own * (n + ALIGN) + own_slot).T)

        def reduce(y):
            return lax.psum_scatter(y, "tp", scatter_dimension=1, tiled=True)

        def swap(y):
            return lax.all_to_all(y, "ep", 0, 0, tiled=True)

        def spare(hall0):
            n = PIECES[0]
            stacked = jax.tree.map(lambda *a: jnp.stack(a), *zip(full_meta, positions, full_rows))

            def body(p, out):
                (meta, spread_meta), pos, own_row = jax.tree.map(lambda a: lax.dynamic_index_in_dim(a, p, 0, False), stacked)
                h = norm_rows(0, n, p.reshape(1), tokens, gain2)
                hall = lax.all_gather(h, "ep", axis=0, tiled=True)
                y = reduce(ffn_piece(1, ep * n, SPARE_TILE, (n, 0), n // CHUNK, meta, pos, hall, w13, w2))
                y = swap(spread_piece(n + ALIGN, ep, spread_meta, y))
                o = mix_piece(n, jnp.stack([col, p]), y, tokens, own_row, gates)
                o = lax.all_gather(o, "tp", axis=1, tiled=True)
                return lax.dynamic_update_slice_in_dim(out, o, p * n, 0)

            return lax.fori_loop(0, len(PIECES), body, unwritten(tokens))

        def fast(level, hall0):
            cap, slots, *tilings = LEVELS[level]
            last, halls, reds, backs, places = None, {0: hall0}, {}, [], []
            for step in ORDER:
                kind, names = step[0], [int(c) for c in step[1:]]
                p = names[0]
                if kind == "A":
                    halls[p] = gather_group(p, normed[p] if last is None else after(normed[p], last))
                elif kind == "F":
                    g, at = home[p]
                    hall = halls[g] if last is None else after(halls[g], last)
                    rows_of, per_block = (sum(GROUPS[g][0]), at), PIECES[p] // CHUNK
                    tile_rows, unroll = tilings[min(p, 1)]
                    last = ffn_piece(unroll, cap, tile_rows, rows_of, per_block, fast_meta[p][level][0], positions[p], hall, w13, w2)
                    reds[p] = reduce(last)
                elif kind == "S":
                    first, parts = next((trip[0], len(trip)) for trip in TRIPS if p in trip)
                    part = p - first
                    meta = fast_meta[p][level][1]
                    last = spread_piece(slots, ep, meta, after(reds[p], last, *backs), part, parts, last if part else None)
                    if p < len(PIECES) - 1:
                        places.append((len(backs), part))
                    if part == parts - 1:
                        backs.append(last)
                        if p < len(PIECES) - 1:
                            backs[-1] = swap(last)
                else:
                    rows = [after(back, last) for back in backs[:-1]]
                    own_rows = jnp.concatenate([fast_rows[q][level] for q in range(len(PIECES))])
                    out = mix_share(tp, places, rows, backs[-1], tokens, own_rows, gates, level)
            return settle(out)

        need = jnp.int32(0)
        for i, (cap, slots, *_) in enumerate(LEVELS):
            over = (functools.reduce(jnp.maximum, most_rows) > cap) | (functools.reduce(jnp.maximum, most_slots) > slots)
            need = jnp.where(over, i + 1, need)
        if mesh.shape["dp"] > 1:
            need = lax.pmax(need, "dp")
        paths = [functools.partial(fast, i) for i in range(len(LEVELS))]
        return lax.switch(need, [*paths, spare], hall0)

    return jax.shard_map(
        local_block,
        mesh=mesh,
        in_specs=(tok_spec, tok_spec, P(None), P(None, None), P("ep", None, "tp"), P("ep", None, "tp"), P("ep", "tp", None)),
        out_specs=tok_spec,
        check_vma=False,
    )
```
